512 devices in a mesh: seq: 64 (over x, z, core), res: 8 (over y).
Axes of the slice: x: 4, y: 8, z: 8, core: 2. Of those that a mesh axis runs over, the one named last changes fastest.
Arguments:
- alignment_rows: bfloat16 [4096, 64, 64], P('seq', 'res'), may hold values from -6 to 6
- pair_features: bfloat16 [64, 64, 128], P('res', 'seq'), may hold values from -6 to 6
- sequence_block_count: int32 [64], P('seq'), may hold values from 16 to 64
- cluster_member_count: int32 [4096], P('seq'), may hold values from 1 to 16
- residue_present_mask: int32 [64], replicated, may hold values 0 or 1
- attention_in_weight: bfloat16 [64, 256], replicated, may hold values from -0.75 to 0.75
- attention_out_weight: bfloat16 [64, 64], replicated, may hold values from -4 to 4
- pair_bias_weight: float32 [128, 8], replicated, may hold values from -48 to 48
- outer_factor_weight: bfloat16 [64, 64], replicated, may hold values from -0.75 to 0.75
- outer_output_weight: float32 [1024, 128], replicated, may hold values from -4 to 4
- outer_product_bias: float32 [128], replicated, may hold values from -3 to 3
Outputs:
- row_attention_update: bfloat16 [4096, 64, 64], P('seq', 'res')
- pair_update: bfloat16 [64, 64, 128], P('seq', 'res')
The draws below stay inside these ranges and needn't reach their ends.
All inputs are finite; a program needn't handle non-finite values.
Results may differ from the reference program's by a relative error of at most 0.0081.
Values may be sent and summed in bfloat16 or wider, within the bound.
No kernel may reach another device: no remote copies, remote signals or barrier semaphores. Data moves between devices by JAX's collectives and lax.ppermute only.
A program may use at most 64 MiB of HBM per device.

```python
import math
import jax
import jax.numpy as jnp
from jax import lax

CHANNEL_COUNT = 64
CP = 128
CO = 32
HEADS = 8
HEAD_DIM = 8
SLOT_DEV = 64
RES_DEV = 8
SLOT_TOTAL = 4096
RESIDUE_TOTAL = 64
N_SEQ = 64
N_RES = 8


def draw_pair_bias_weight(key, part):
    values = jax.random.normal(key, (CP, HEADS), jnp.float32) * (2.0 / math.sqrt(CP))
    return jnp.clip(values, -48.0, 48.0)


def plant(values, key, low, top_value):
    index_at = [jax.random.randint(jax.random.fold_in(key, axis), (), 0, length) for axis, length in enumerate(values.shape)]
    widest = values.shape.index(max(values.shape))
    neighbour = index_at[:widest] + [(index_at[widest] + 1) % values.shape[widest]] + index_at[widest + 1:]
    return values.at[tuple(index_at)].set(low).at[tuple(neighbour)].set(top_value)


def level_of(key, shape, split, low, high):
    level = 1.0
    for position, blocks in split:
        steps = jax.random.uniform(jax.random.fold_in(jax.random.fold_in(key, 6), position), (blocks,), jnp.float32, low / len(split), high / len(split))
        level = level * jnp.repeat(jnp.exp(steps), shape[position] // blocks).reshape((-1,) + (1,) * (len(shape) - 1 - position))
    return level


def centred(rng, dims, scale, reach, split=(), kind=jnp.bfloat16):
    drawn = jax.random.normal(rng, dims, jnp.float32) * scale
    if len(split) > 0:
        drawn = level_of(rng, dims, split, -0.22, 0.18) * drawn
    return jnp.clip(drawn, min=-reach, max=reach).astype(kind)


def setup_inputs(seed: int = 0) -> dict:
    arg_keys = jax.random.split(jax.random.key(seed), 12)
    return {
        "alignment_rows": centred(arg_keys[0], (SLOT_TOTAL, RESIDUE_TOTAL, CHANNEL_COUNT), 1.0, 6.0, ((0, 64), (1, 8))),
        "pair_features": centred(arg_keys[1], (RESIDUE_TOTAL, RESIDUE_TOTAL, CP), 1.0, 6.0, ((0, 8), (1, 64))),
        "sequence_block_count": plant(jax.random.randint(arg_keys[2], (N_SEQ,), SLOT_DEV // 4, SLOT_DEV + 1), jax.random.fold_in(arg_keys[2], 1), SLOT_DEV // 4, SLOT_DEV).astype(jnp.int32),
        "cluster_member_count": plant(jax.random.randint(arg_keys[3], (SLOT_TOTAL,), 1, 17), jax.random.fold_in(arg_keys[3], 1), 1, 16).astype(jnp.int32),
        "residue_present_mask": plant((jax.random.randint(arg_keys[4], (RESIDUE_TOTAL,), 0, 8) < 7).astype(jnp.int32), jax.random.fold_in(arg_keys[4], 1), 0, 1),
        "attention_in_weight": centred(arg_keys[5], (CHANNEL_COUNT, 4 * CHANNEL_COUNT), CHANNEL_COUNT ** -0.5, 0.75),
        "attention_out_weight": centred(arg_keys[6], (CHANNEL_COUNT, CHANNEL_COUNT), 1.0, 4.0),
        "pair_bias_weight": draw_pair_bias_weight(jax.random.fold_in(arg_keys[11], 71), 0),
        "outer_factor_weight": centred(arg_keys[8], (CHANNEL_COUNT, 2 * CO), CHANNEL_COUNT ** -0.5, 0.75),
        "outer_output_weight": centred(arg_keys[9], (CO * CO, CP), 1.0, 4.0, (), jnp.float32),
        "outer_product_bias": centred(arg_keys[10], (CP,), 0.5, 3.0, (), jnp.float32),
    }


def apply_layer_norm(values):
    centre = lax.optimization_barrier(jnp.mean(values, axis=-1, keepdims=True))
    spread = lax.optimization_barrier(jnp.mean(jnp.square(values - centre), axis=-1, keepdims=True))
    return (values - centre) * lax.rsqrt(spread + 1e-05)

def attend_block(pieces, full_bias):
    query_rows, key_value_pairs, gate_activation = pieces
    slot_count, n_query, channel_width = query_rows.shape
    head_count = full_bias.shape[0]
    head_dim = channel_width // head_count
    n_keys = key_value_pairs.shape[1]
    query_heads = query_rows.astype(jnp.float32).reshape(slot_count, n_query, head_count, head_dim)
    key_heads = key_value_pairs[..., :channel_width].astype(jnp.float32).reshape(slot_count, n_keys, head_count, head_dim)
    value_heads = key_value_pairs[..., channel_width:].astype(jnp.float32).reshape(slot_count, n_keys, head_count, head_dim)
    scores = jnp.einsum('bihd,bjhd->bhij', query_heads, key_heads, precision=lax.Precision.HIGHEST) + full_bias[None]
    row_max = lax.optimization_barrier(jnp.max(scores, axis=-1, keepdims=True))
    expo = jnp.exp(scores - row_max)
    probs = (expo / lax.optimization_barrier(jnp.sum(expo, axis=-1, keepdims=True))).astype(jnp.bfloat16)
    context = jnp.einsum('bhij,bjhd->bihd', probs.astype(jnp.float32), value_heads, precision=lax.Precision.HIGHEST)
    return (gate_activation * context.reshape(slot_count, n_query, channel_width)).astype(jnp.bfloat16)

def reference(alignment_rows, pair_features, sequence_block_count, cluster_member_count, residue_present_mask, attention_in_weight, attention_out_weight, pair_bias_weight, outer_factor_weight, outer_output_weight, outer_product_bias):
    total_count = SLOT_DEV * N_SEQ
    block_length = RES_DEV * N_RES
    slot_ids = jnp.arange(total_count, dtype=jnp.int32)
    usable = (slot_ids % SLOT_DEV < sequence_block_count[slot_ids // SLOT_DEV]).astype(jnp.float32)
    seq_weight = cluster_member_count.astype(jnp.float32) * usable
    weight_sum = jnp.sum(seq_weight)
    key_mask = jnp.where(residue_present_mask == 1, 0.0, -1000000.0).astype(jnp.float32)
    pair_norm = apply_layer_norm(pair_features.astype(jnp.float32))
    pair_bias = jnp.einsum('ijp,ph->hij', pair_norm, pair_bias_weight, precision=lax.Precision.HIGHEST) + key_mask[None, None, :]
    normed_alignment = apply_layer_norm(alignment_rows.astype(jnp.float32)).astype(jnp.bfloat16)
    projected_rows = jnp.dot(normed_alignment.reshape(-1, CHANNEL_COUNT), attention_in_weight, preferred_element_type=jnp.float32).reshape(total_count, block_length, 4 * CHANNEL_COUNT)
    query_rows = (projected_rows[..., :CHANNEL_COUNT] * (1.0 / math.sqrt(HEAD_DIM))).astype(jnp.bfloat16)
    key_value_pairs = projected_rows[..., CHANNEL_COUNT:3 * CHANNEL_COUNT].astype(jnp.bfloat16)
    gate_activation = jax.nn.sigmoid(projected_rows[..., 3 * CHANNEL_COUNT:])
    gated = lax.map(lambda pieces: attend_block(pieces, pair_bias), (query_rows.reshape(N_SEQ, SLOT_DEV, block_length, CHANNEL_COUNT), key_value_pairs.reshape(N_SEQ, SLOT_DEV, block_length, 2 * CHANNEL_COUNT), gate_activation.reshape(N_SEQ, SLOT_DEV, block_length, CHANNEL_COUNT)))
    update = jnp.dot(gated.reshape(-1, CHANNEL_COUNT), attention_out_weight, preferred_element_type=jnp.float32).astype(jnp.bfloat16)
    row_attention_update = update.reshape(total_count, block_length, CHANNEL_COUNT) * usable.astype(jnp.bfloat16)[:, None, None]
    updated_alignment = alignment_rows.astype(jnp.float32) + row_attention_update.astype(jnp.float32)
    outer_input_norm = apply_layer_norm(updated_alignment).astype(jnp.bfloat16)
    factors = jnp.dot(outer_input_norm.reshape(-1, CHANNEL_COUNT), outer_factor_weight, preferred_element_type=jnp.float32).reshape(total_count, block_length, 2 * CO)
    res_keep = residue_present_mask.astype(jnp.float32)[None, :, None]
    left_proj = (factors[..., :CO] * res_keep).astype(jnp.bfloat16)
    right_proj = (factors[..., CO:] * res_keep * seq_weight[:, None, None]).astype(jnp.bfloat16)
    outer = lax.dot_general(left_proj.reshape(total_count, block_length * CO).astype(jnp.float32), right_proj.reshape(total_count, block_length * CO).astype(jnp.float32), (((0,), (0,)), ((), ())), precision=lax.Precision.HIGHEST)
    outer = outer.reshape(block_length, CO, block_length, CO)
    projected = jnp.einsum('icjd,cdp->ijp', outer, outer_output_weight.reshape(CO, CO, CP), precision=lax.Precision.HIGHEST)
    pair_update = (projected / weight_sum + outer_product_bias).astype(jnp.bfloat16)
    return (row_attention_update, pair_update)
```

```python
import functools
import math

import jax
import jax.numpy as jnp
from jax import lax
from jax.experimental import pallas as pl
from jax.experimental.pallas import tpu as pltpu
from jax.sharding import PartitionSpec as P

BF = jnp.bfloat16
F32 = jnp.float32
VMEM = pl.BlockSpec(memory_space=pltpu.VMEM)
SMEM = pl.BlockSpec(memory_space=pltpu.SMEM)


def dot(a, b):
    return jnp.dot(a, b, preferred_element_type=F32)


def dot_nt(a, b):
    return lax.dot_general(a, b, (((1,), (1,)), ((), ())), preferred_element_type=F32)


def dot_tn(a, b):
    return lax.dot_general(a, b, (((0,), (0,)), ((), ())), preferred_element_type=F32)


def dot_split(x, matrix):
    high = x.astype(BF)
    low = (x - high.astype(F32)).astype(BF)
    return dot(high, matrix) + dot(low, matrix)


def averager(width):
    row = lax.broadcasted_iota(jnp.int32, (width, width), 0) // 64
    col = lax.broadcasted_iota(jnp.int32, (width, width), 1) // 64
    return jnp.where(row == col, 1.0 / 64, 0.0).astype(BF)


def norm_groups(x, matrix):
    centred = x - dot_split(x, matrix)
    spread = dot_split(centred * centred, matrix)
    return centred * lax.rsqrt(spread + 1e-05)


def block_diagonal(weight):
    wide = jnp.concatenate([weight.astype(F32)] * 4, axis=1)
    full = jnp.concatenate([wide] * 4, axis=0)
    row = lax.broadcasted_iota(jnp.int32, full.shape, 0) // 64
    col = lax.broadcasted_iota(jnp.int32, full.shape, 1) // 64
    return jnp.where(row == col, full, 0.0).astype(BF)


def prepare_kernel(where_ref, count_ref, mask_ref, rows_ref, pair_ref, bias_w_ref, members_ref,
                   bias_out, send_out, own_out, rows_out):
    pair = pair_ref[...].astype(F32)
    pair = pair - jnp.mean(pair, axis=-1, keepdims=True)
    pair = pair * lax.rsqrt(jnp.mean(pair * pair, axis=-1, keepdims=True) + 1e-05)
    products = bias_w_ref[...][:, None, :] * pair[None, :, :]
    column = jnp.sum(products, axis=-1, keepdims=True).reshape(64, 1)
    row = lax.broadcasted_iota(jnp.int32, (64, 128), 0)
    lane = lax.broadcasted_iota(jnp.int32, (64, 128), 1)
    bias = jnp.sum(jnp.where(row == lane, column, 0.0), axis=0, keepdims=True)
    bias = bias + jnp.where(mask_ref[where_ref[0]] == 1, 0.0, -1000000.0)
    slot = lax.broadcasted_iota(jnp.int32, (1, 64), 1)
    weight = jnp.where(slot < count_ref[0], members_ref[...], 0).astype(F32)
    bias = jnp.where(lane[:1] < 64, bias, jnp.sum(weight))
    bias_out[...] = jnp.broadcast_to(bias[None], (64, 1, 128))

    rows = rows_ref[...].astype(F32)
    low = jnp.concatenate([rows[0:16], rows[16:32]], axis=-1)
    high = jnp.concatenate([rows[32:48], rows[48:64]], axis=-1)
    x = jnp.concatenate([low, high], axis=-1).reshape(128, 256)
    rows_out[...] = x
    normed = norm_groups(x, averager(256))
    own_out[...] = normed.astype(BF)
    block = normed.reshape(16, 8, 256).astype(BF)
    for peer in range(8):
        send_out[peer] = block


def project_kernel(own_ref, in_w_ref, out_w_ref, q_out, gate_out, k_out, v_out, o_out):
    weight = in_w_ref[...]
    own = own_ref[...]
    q_out[...] = dot(own, block_diagonal(weight[:, 0:64])) * (1.0 / math.sqrt(8))
    gate_out[...] = jax.nn.sigmoid(dot(own, block_diagonal(weight[:, 192:256])))
    k_out[...] = block_diagonal(weight[:, 64:128])
    v_out[...] = block_diagonal(weight[:, 128:192])
    o_out[...] = block_diagonal(out_w_ref[...])


GROUPS = 4


def attend_kernel(where_ref, count_ref, mask_ref, all_ref, bias_ref, q_ref, gate_ref, rows_ref,
                  k_w_ref, v_w_ref, o_w_ref, factor_ref, members_ref,
                  update_out, left_out, right_out,
                  x_scr, k_scr, v_scr, context_scr, norm_scr, left_scr):
    lane = lax.broadcasted_iota(jnp.int32, (64, 128), 1)
    bias = bias_ref[...]
    bias = jnp.where(lane < 64, bias, pltpu.roll(bias, 64, axis=1))
    for g in range(16):
        x_scr[g] = all_ref[:, g].astype(F32).reshape(64, 256).astype(BF)
    x = x_scr[...].reshape(1024, 256)
    k_scr[...] = dot(x, k_w_ref[...]).astype(BF).reshape(16, 64, 256)
    v_scr[...] = dot(x, v_w_ref[...]).astype(BF).reshape(16, 64, 256)
    diagonal = (lax.broadcasted_iota(jnp.int32, (16, 8, 128), 2) // 8
                == lax.broadcasted_iota(jnp.int32, (16, 8, 128), 0))

    def some_groups(step, carry):
        first = step * GROUPS
        parts = [(n, h) for n in range(GROUPS) for h in range(2)]
        scores = []
        for n, h in parts:
            start = pl.multiple_of((first + n) * 8, 8)
            q = q_ref[pl.ds(start, 8), h * 128:(h + 1) * 128]
            q = jnp.where(diagonal, q[None], 0.0).reshape(128, 128).astype(BF)
            k = k_scr[first + n, :, h * 128:(h + 1) * 128]
            scores.append(dot_nt(k, q) + bias)
        probs = []
        for s in scores:
            e = jnp.exp(s - jnp.max(s, axis=0, keepdims=True))
            probs.append((e * (1.0 / jnp.sum(e, axis=0, keepdims=True))).astype(BF))
        for (n, h), p in zip(parts, probs):
            start = pl.multiple_of((first + n) * 8, 8)
            v = v_scr[first + n, :, h * 128:(h + 1) * 128]
            full = dot_tn(p, v).reshape(16, 8, 128)
            context_scr[pl.ds(start, 8), h * 128:(h + 1) * 128] = jnp.sum(
                jnp.where(diagonal, full, 0.0), axis=0)
        return carry

    lax.fori_loop(0, 16 // GROUPS, some_groups, 0)

    gated = (gate_ref[...] * context_scr[...]).astype(BF)
    update = dot(gated, o_w_ref[...]).astype(BF).astype(F32)
    slot = (lax.broadcasted_iota(jnp.int32, (128, 256), 1) // 64 * 16
            + lax.broadcasted_iota(jnp.int32, (128, 256), 0) // 8)
    update = update * (slot < count_ref[0]).astype(F32)
    cube = update.reshape(16, 8, 256)
    for q in range(4):
        update_out[q * 16:(q + 1) * 16] = cube[:, :, q * 64:(q + 1) * 64].astype(BF)

    full_norm = norm_groups(rows_ref[...] + update, averager(256))
    norm_scr[0] = full_norm[:, :128]
    norm_scr[1] = full_norm[:, 128:]
    pieces = []
    for i in range(8):
        for half in range(2):
            z = norm_scr[half, pl.ds(i, 16, stride=8), :]
            pieces += [z, pltpu.roll(z, 64, axis=1)]
    tokens = jnp.concatenate(pieces, axis=0).astype(BF)

    factor = factor_ref[...].astype(F32)
    zero = jnp.zeros((64, 128), F32)
    right_w = jnp.concatenate([jnp.concatenate([factor[:, 32:64]] * 4, axis=1), zero], axis=0)
    right = dot(tokens, right_w.astype(BF))
    base = where_ref[1] * 8
    kept = []
    for j in range(8):
        keep = (mask_ref[base + j]).astype(F32)
        kept.append(right[j * 64:(j + 1) * 64] * keep)
    for quad in range(2):
        a, b, c, d = kept[quad * 4:quad * 4 + 4]
        r = jnp.where(lane < 64, jnp.where(lane < 32, a, b), jnp.where(lane < 96, c, d))
        right_out[:, quad * 128:(quad + 1) * 128] = r.astype(BF)

    left_w = jnp.concatenate([factor.T[0:32], jnp.zeros((32, 64), F32)], axis=1).astype(BF)
    left = dot_nt(left_w, tokens)
    members = members_ref[...]
    members = jnp.concatenate([members, members], axis=1)
    lane1 = lax.broadcasted_iota(jnp.int32, (1, 128), 1)
    weight = jnp.where(lane1 % 64 < count_ref[0], members, 0).astype(F32)
    lane32 = lax.broadcasted_iota(jnp.int32, (32, 128), 1)
    for pair in range(4):
        both = left[:, pair * 128:(pair + 1) * 128]
        turned = pltpu.roll(both, 64, axis=1)
        for odd in range(2):
            i = pair * 2 + odd
            keep = (mask_ref[base + i]).astype(F32)
            mine = jnp.where((lane32 < 64) == (odd == 0), both, turned)
            left_scr[i * 32:(i + 1) * 32, :] = mine * (weight * keep)
    rows = []
    lane8 = lax.broadcasted_iota(jnp.int32, (8, 128), 1)
    for c in range(16):
        rows.append(jnp.where(lane8 < 64, left_scr[pl.ds(2 * c, 8, stride=32), :],
                              left_scr[pl.ds(2 * c + 1, 8, stride=32), :]))
    block = jnp.concatenate(rows, axis=0).astype(BF)
    for peer in range(8):
        left_out[peer] = block


def outer_kernel(left_ref, right_ref, weight_ref, out_ref, outer_scr, part_scr):
    right = right_ref[...]
    zero = jnp.zeros_like(right)
    both = jnp.concatenate([jnp.concatenate([right, zero], axis=1),
                            jnp.concatenate([zero, right], axis=1)], axis=0)
    outer_scr[...] = dot(left_ref[...].reshape(1024, 128), both).reshape(8, 16, 8, 512)
    weight = weight_ref[...].astype(BF)
    lane = lax.broadcasted_iota(jnp.int32, (64, 128), 1)
    for quad in range(2):
        rows = [[] for _ in range(4)]
        for m in range(8):
            pieces = []
            for k in range(4):
                c, odd = 2 * m + k // 2, k % 2
                lanes = odd * 256 + quad * 128
                pieces.append(outer_scr[:, c, :, lanes:lanes + 128].reshape(64, 128))
            for j in range(4):
                turned = [pltpu.roll(p, (k - j) * 32 % 128, axis=1) if k != j else p
                          for k, p in enumerate(pieces)]
                low = jnp.where(lane < 32, turned[0], turned[1])
                high = jnp.where(lane < 96, turned[2], turned[3])
                rows[j].append(jnp.where(lane < 64, low, high).astype(BF))
        for j in range(4):
            part = dot(jnp.concatenate(rows[j], axis=1), weight)
            part_scr[pl.ds(quad * 4 + j, 64, stride=8), :] = part
    out_ref[...] = part_scr[...].reshape(64, 8, 128).astype(BF)


def call(kernel, outs, specs, scratch=(), flops=0):
    return pl.pallas_call(
        kernel,
        out_shape=[jax.ShapeDtypeStruct(shape, kind) for shape, kind in outs],
        in_specs=specs,
        out_specs=[VMEM] * len(outs),
        scratch_shapes=[pltpu.VMEM(shape, kind) for shape, kind in scratch],
        cost_estimate=pl.CostEstimate(flops=flops, bytes_accessed=1 << 20, transcendentals=0),
    )


def local(
    alignment_rows,
    pair_features,
    sequence_block_count,
    cluster_member_count,
    residue_present_mask,
    attention_in_weight,
    attention_out_weight,
    pair_bias_weight,
    outer_factor_weight,
    outer_output_weight,
    outer_product_bias,
):
    here = jnp.stack([lax.axis_index("seq"), lax.axis_index("res")]).astype(jnp.int32)
    members = cluster_member_count.reshape(1, 64)
    bias_send, rows_send, own_norm, own_rows = call(
        prepare_kernel,
        [((64, 1, 128), F32), ((8, 16, 8, 256), BF), ((128, 256), BF), ((128, 256), F32)],
        [SMEM] * 3 + [VMEM] * 4,
    )(here, sequence_block_count, residue_present_mask, alignment_rows,
      pair_features.reshape(8, 128), pair_bias_weight.T, members)
    rows_all = lax.all_to_all(rows_send, "res", split_axis=0, concat_axis=0, tiled=True)
    bias_all = lax.all_to_all(bias_send, "seq", split_axis=0, concat_axis=0, tiled=True)
    bias_all = bias_all.reshape(64, 128)
    queries, gate, k_w, v_w, o_w = call(
        project_kernel,
        [((128, 256), F32), ((128, 256), F32)] + [((256, 256), BF)] * 3,
        [VMEM] * 3,
        flops=1 << 30,
    )(own_norm, attention_in_weight, attention_out_weight)
    row_attention_update, left_send, right = call(
        attend_kernel,
        [((64, 8, 64), BF), ((8, 128, 128), BF), ((64, 256), BF)],
        [SMEM] * 3 + [VMEM] * 10,
        [((16, 64, 256), BF)] * 3
        + [((128, 256), F32), ((2, 128, 128), F32), ((256, 128), F32)],
    )(here, sequence_block_count, residue_present_mask, rows_all, bias_all, queries, gate,
      own_rows, k_w, v_w, o_w, outer_factor_weight, members)
    left_all = lax.all_to_all(left_send, "res", split_axis=0, concat_axis=0, tiled=True)
    (partial,) = call(
        outer_kernel,
        [((64, 8, 128), BF)],
        [VMEM] * 3,
        [((8, 16, 8, 512), F32), ((512, 128), F32)],
    )(left_all, right, outer_output_weight)
    arrived = lax.all_to_all(partial, "seq", split_axis=0, concat_axis=0, tiled=True)
    summed = arrived.astype(F32).sum(axis=0)
    weight_sum = jnp.sum(bias_all[:, 64])
    pair_update = (summed / weight_sum + outer_product_bias).astype(BF)
    return (row_attention_update, pair_update[None])


def solution(mesh):
    return jax.shard_map(
        local,
        mesh=mesh,
        in_specs=(
            P("seq", "res", None),
            P("res", "seq", None),
            P("seq"),
            P("seq"),
            P(),
            P(),
            P(),
            P(),
            P(),
            P(),
            P(),
        ),
        out_specs=(P("seq", "res", None), P("seq", "res", None)),
        check_vma=False,
    )
```

```python
import functools
import math

import jax
import jax.numpy as jnp
from jax import lax
from jax.experimental import pallas as pl
from jax.experimental.pallas import tpu as pltpu
from jax.sharding import PartitionSpec as P

BF = jnp.bfloat16
F32 = jnp.float32
VMEM = pl.BlockSpec(memory_space=pltpu.VMEM)
SMEM = pl.BlockSpec(memory_space=pltpu.SMEM)


def dot(a, b):
    return jnp.dot(a, b, preferred_element_type=F32)


def dot_nt(a, b):
    return lax.dot_general(a, b, (((1,), (1,)), ((), ())), preferred_element_type=F32)


def dot_tn(a, b):
    return lax.dot_general(a, b, (((0,), (0,)), ((), ())), preferred_element_type=F32)


def dot_split(x, matrix):
    high = x.astype(BF)
    low = (x - high.astype(F32)).astype(BF)
    return dot(high, matrix) + dot(low, matrix)


def averager(width):
    row = lax.broadcasted_iota(jnp.int32, (width, width), 0) // 64
    col = lax.broadcasted_iota(jnp.int32, (width, width), 1) // 64
    return jnp.where(row == col, 1.0 / 64, 0.0).astype(BF)


def norm_groups(x, matrix):
    centred = x - dot_split(x, matrix)
    spread = dot_split(centred * centred, matrix)
    return centred * lax.rsqrt(spread + 1e-05)


def block_diagonal(weight):
    wide = jnp.concatenate([weight.astype(F32)] * 4, axis=1)
    full = jnp.concatenate([wide] * 4, axis=0)
    row = lax.broadcasted_iota(jnp.int32, full.shape, 0) // 64
    col = lax.broadcasted_iota(jnp.int32, full.shape, 1) // 64
    return jnp.where(row == col, full, 0.0).astype(BF)


def prepare_kernel(count_ref, mask_ref, rows_ref, pair_ref, bias_w_ref, members_ref,
                   bias_out, send_out, own_out, rows_out):
    pair = pair_ref[...].astype(F32)
    pair = pair - jnp.mean(pair, axis=-1, keepdims=True)
    pair = pair * lax.rsqrt(jnp.mean(pair * pair, axis=-1, keepdims=True) + 1e-05)
    products = bias_w_ref[...][:, None, :] * pair[None, :, :]
    column = jnp.sum(products, axis=-1, keepdims=True).reshape(64, 1)
    row = lax.broadcasted_iota(jnp.int32, (64, 128), 0)
    lane = lax.broadcasted_iota(jnp.int32, (64, 128), 1)
    bias = jnp.sum(jnp.where(row == lane, column, 0.0), axis=0, keepdims=True)
    bias = bias + jnp.where(mask_ref[lax.axis_index("seq")] == 1, 0.0, -1000000.0)
    slot = lax.broadcasted_iota(jnp.int32, (1, 64), 1)
    weight = jnp.where(slot < count_ref[0], members_ref[...], 0).astype(F32)
    bias = jnp.where(lane[:1] < 64, bias, jnp.sum(weight))
    bias_out[...] = jnp.broadcast_to(bias[None], (64, 1, 128))

    rows = rows_ref[...].astype(F32)
    low = jnp.concatenate([rows[0:16], rows[16:32]], axis=-1)
    high = jnp.concatenate([rows[32:48], rows[48:64]], axis=-1)
    x = jnp.concatenate([low, high], axis=-1).reshape(128, 256)
    rows_out[...] = x
    normed = norm_groups(x, averager(256))
    own_out[...] = normed.astype(BF)
    block = normed.reshape(16, 8, 256).astype(BF)
    for peer in range(8):
        send_out[peer] = block


def project_kernel(own_ref, in_w_ref, out_w_ref, q_out, gate_out, k_out, v_out, o_out):
    weight = in_w_ref[...]
    own = own_ref[...]
    q_out[...] = dot(own, block_diagonal(weight[:, 0:64])) * (1.0 / math.sqrt(8))
    gate_out[...] = jax.nn.sigmoid(dot(own, block_diagonal(weight[:, 192:256])))
    k_out[...] = block_diagonal(weight[:, 64:128])
    v_out[...] = block_diagonal(weight[:, 128:192])
    o_out[...] = block_diagonal(out_w_ref[...])


GROUPS = 4


def attend_kernel(count_ref, mask_ref, all_ref, bias_ref, q_ref, gate_ref, rows_ref,
                  k_w_ref, v_w_ref, o_w_ref, factor_ref, members_ref,
                  update_out, left_out, right_out,
                  x_scr, k_scr, v_scr, context_scr, norm_scr, left_scr):
    lane = lax.broadcasted_iota(jnp.int32, (64, 128), 1)
    bias = bias_ref[...]
    bias = jnp.where(lane < 64, bias, pltpu.roll(bias, 64, axis=1))
    for g in range(16):
        x_scr[g] = all_ref[:, g].astype(F32).reshape(64, 256).astype(BF)
    x = x_scr[...].reshape(1024, 256)
    k_scr[...] = dot(x, k_w_ref[...]).astype(BF).reshape(16, 64, 256)
    v_scr[...] = dot(x, v_w_ref[...]).astype(BF).reshape(16, 64, 256)
    diagonal = (lax.broadcasted_iota(jnp.int32, (16, 8, 128), 2) // 8
                == lax.broadcasted_iota(jnp.int32, (16, 8, 128), 0))

    def some_groups(step, carry):
        first = step * GROUPS
        parts = [(n, h) for n in range(GROUPS) for h in range(2)]
        scores = []
        for n, h in parts:
            start = pl.multiple_of((first + n) * 8, 8)
            q = q_ref[pl.ds(start, 8), h * 128:(h + 1) * 128]
            q = jnp.where(diagonal, q[None], 0.0).reshape(128, 128).astype(BF)
            k = k_scr[first + n, :, h * 128:(h + 1) * 128]
            scores.append(dot_nt(k, q) + bias)
        probs = []
        for s in scores:
            e = jnp.exp(s - jnp.max(s, axis=0, keepdims=True))
            probs.append((e * (1.0 / jnp.sum(e, axis=0, keepdims=True))).astype(BF))
        for (n, h), p in zip(parts, probs):
            start = pl.multiple_of((first + n) * 8, 8)
            v = v_scr[first + n, :, h * 128:(h + 1) * 128]
            full = dot_tn(p, v).reshape(16, 8, 128)
            context_scr[pl.ds(start, 8), h * 128:(h + 1) * 128] = jnp.sum(
                jnp.where(diagonal, full, 0.0), axis=0)
        return carry

    lax.fori_loop(0, 16 // GROUPS, some_groups, 0)

    gated = (gate_ref[...] * context_scr[...]).astype(BF)
    update = dot(gated, o_w_ref[...]).astype(BF).astype(F32)
    slot = (lax.broadcasted_iota(jnp.int32, (128, 256), 1) // 64 * 16
            + lax.broadcasted_iota(jnp.int32, (128, 256), 0) // 8)
    update = update * (slot < count_ref[0]).astype(F32)
    cube = update.reshape(16, 8, 256)
    for q in range(4):
        update_out[q * 16:(q + 1) * 16] = cube[:, :, q * 64:(q + 1) * 64].astype(BF)

    full_norm = norm_groups(rows_ref[...] + update, averager(256))
    norm_scr[0] = full_norm[:, :128]
    norm_scr[1] = full_norm[:, 128:]
    pieces = []
    for i in range(8):
        for half in range(2):
            z = norm_scr[half, pl.ds(i, 16, stride=8), :]
            pieces += [z, pltpu.roll(z, 64, axis=1)]
    tokens = jnp.concatenate(pieces, axis=0).astype(BF)

    factor = factor_ref[...].astype(F32)
    zero = jnp.zeros((64, 128), F32)
    right_w = jnp.concatenate([jnp.concatenate([factor[:, 32:64]] * 4, axis=1), zero], axis=0)
    right = dot(tokens, right_w.astype(BF))
    base = lax.axis_index("res") * 8
    kept = []
    for j in range(8):
        keep = (mask_ref[base + j]).astype(F32)
        kept.append(right[j * 64:(j + 1) * 64] * keep)
    for quad in range(2):
        a, b, c, d = kept[quad * 4:quad * 4 + 4]
        r = jnp.where(lane < 64, jnp.where(lane < 32, a, b), jnp.where(lane < 96, c, d))
        right_out[:, quad * 128:(quad + 1) * 128] = r.astype(BF)

    left_w = jnp.concatenate([factor.T[0:32], jnp.zeros((32, 64), F32)], axis=1).astype(BF)
    left = dot_nt(left_w, tokens)
    members = members_ref[...]
    members = jnp.concatenate([members, members], axis=1)
    lane1 = lax.broadcasted_iota(jnp.int32, (1, 128), 1)
    weight = jnp.where(lane1 % 64 < count_ref[0], members, 0).astype(F32)
    lane32 = lax.broadcasted_iota(jnp.int32, (32, 128), 1)
    for pair in range(4):
        both = left[:, pair * 128:(pair + 1) * 128]
        turned = pltpu.roll(both, 64, axis=1)
        for odd in range(2):
            i = pair * 2 + odd
            keep = (mask_ref[base + i]).astype(F32)
            mine = jnp.where((lane32 < 64) == (odd == 0), both, turned)
            left_scr[i * 32:(i + 1) * 32, :] = mine * (weight * keep)
    rows = []
    lane8 = lax.broadcasted_iota(jnp.int32, (8, 128), 1)
    for c in range(16):
        rows.append(jnp.where(lane8 < 64, left_scr[pl.ds(2 * c, 8, stride=32), :],
                              left_scr[pl.ds(2 * c + 1, 8, stride=32), :]))
    block = jnp.concatenate(rows, axis=0).astype(BF)
    for peer in range(8):
        left_out[peer] = block


def outer_kernel(left_ref, right_ref, weight_ref, out_ref, outer_scr, part_scr):
    right = right_ref[...]
    zero = jnp.zeros_like(right)
    both = jnp.concatenate([jnp.concatenate([right, zero], axis=1),
                            jnp.concatenate([zero, right], axis=1)], axis=0)
    outer_scr[...] = dot(left_ref[...].reshape(1024, 128), both).reshape(8, 16, 8, 512)
    weight = weight_ref[...].astype(BF)
    lane = lax.broadcasted_iota(jnp.int32, (64, 128), 1)
    for quad in range(2):
        rows = [[] for _ in range(4)]
        for m in range(8):
            pieces = []
            for k in range(4):
                c, odd = 2 * m + k // 2, k % 2
                lanes = odd * 256 + quad * 128
                pieces.append(outer_scr[:, c, :, lanes:lanes + 128].reshape(64, 128))
            for j in range(4):
                turned = [pltpu.roll(p, (k - j) * 32 % 128, axis=1) if k != j else p
                          for k, p in enumerate(pieces)]
                low = jnp.where(lane < 32, turned[0], turned[1])
                high = jnp.where(lane < 96, turned[2], turned[3])
                rows[j].append(jnp.where(lane < 64, low, high).astype(BF))
        for j in range(4):
            part = dot(jnp.concatenate(rows[j], axis=1), weight)
            part_scr[pl.ds(quad * 4 + j, 64, stride=8), :] = part
    out_ref[...] = part_scr[...].reshape(64, 8, 128).astype(BF)


def call(kernel, outs, specs, scratch=(), flops=0, limit=8):
    return pl.pallas_call(
        kernel,
        out_shape=[jax.ShapeDtypeStruct(shape, kind) for shape, kind in outs],
        in_specs=specs,
        out_specs=[VMEM] * len(outs),
        scratch_shapes=[pltpu.VMEM(shape, kind) for shape, kind in scratch],
        cost_estimate=pl.CostEstimate(flops=flops, bytes_accessed=1 << 20, transcendentals=0),
        compiler_params=pltpu.CompilerParams(vmem_limit_bytes=limit << 20),
    )


def local(
    alignment_rows,
    pair_features,
    sequence_block_count,
    cluster_member_count,
    residue_present_mask,
    attention_in_weight,
    attention_out_weight,
    pair_bias_weight,
    outer_factor_weight,
    outer_output_weight,
    outer_product_bias,
):
    members = cluster_member_count.reshape(1, 64)
    bias_send, rows_send, own_norm, own_rows = call(
        prepare_kernel,
        [((64, 1, 128), F32), ((8, 16, 8, 256), BF), ((128, 256), BF), ((128, 256), F32)],
        [SMEM] * 2 + [VMEM] * 4,
    )(sequence_block_count, residue_present_mask, alignment_rows,
      pair_features.reshape(8, 128), pair_bias_weight.T, members)
    bias_all = lax.all_to_all(bias_send, "seq", split_axis=0, concat_axis=0, tiled=True)
    rows_all = lax.all_to_all(rows_send, "res", split_axis=0, concat_axis=0, tiled=True)
    bias_all = bias_all.reshape(64, 128)
    queries, gate, k_w, v_w, o_w = call(
        project_kernel,
        [((128, 256), F32), ((128, 256), F32)] + [((256, 256), BF)] * 3,
        [VMEM] * 3,
        flops=1 << 30,
    )(own_norm, attention_in_weight, attention_out_weight)
    row_attention_update, left_send, right = call(
        attend_kernel,
        [((64, 8, 64), BF), ((8, 128, 128), BF), ((64, 256), BF)],
        [SMEM] * 2 + [VMEM] * 10,
        [((16, 64, 256), BF)] * 3
        + [((128, 256), F32), ((2, 128, 128), F32), ((256, 128), F32)],
    )(sequence_block_count, residue_present_mask, rows_all, bias_all, queries, gate,
      own_rows, k_w, v_w, o_w, outer_factor_weight, members)
    left_all = lax.all_to_all(left_send, "res", split_axis=0, concat_axis=0, tiled=True)
    (partial,) = call(
        outer_kernel,
        [((64, 8, 128), BF)],
        [VMEM] * 3,
        [((8, 16, 8, 512), F32), ((512, 128), F32)],
    )(left_all, right, outer_output_weight)
    arrived = lax.all_to_all(partial, "seq", split_axis=0, concat_axis=0, tiled=True)
    summed = arrived.astype(F32).sum(axis=0)
    weight_sum = jnp.sum(bias_all[:, 64])
    pair_update = (summed / weight_sum + outer_product_bias).astype(BF)
    return (row_attention_update, pair_update[None])


def solution(mesh):
    return jax.shard_map(
        local,
        mesh=mesh,
        in_specs=(
            P("seq", "res", None),
            P("res", "seq", None),
            P("seq"),
            P("seq"),
            P(),
            P(),
            P(),
            P(),
            P(),
            P(),
            P(),
        ),
        out_specs=(P("seq", "res", None), P("seq", "res", None)),
        check_vma=False,
    )
```

```python
import math

import jax
import jax.numpy as jnp
from jax import lax
from jax.experimental import pallas as pl
from jax.experimental.pallas import tpu as pltpu
from jax.sharding import PartitionSpec as P

BF = jnp.bfloat16
F32 = jnp.float32
VMEM = pl.BlockSpec(memory_space=pltpu.VMEM)
SMEM = pl.BlockSpec(memory_space=pltpu.SMEM)
HBM = pl.BlockSpec(memory_space=pltpu.HBM)


def dot(a, b):
    return jnp.dot(a, b, preferred_element_type=F32)


def dot_nt(a, b):
    return lax.dot_general(a, b, (((1,), (1,)), ((), ())), preferred_element_type=F32)


def dot_tn(a, b):
    return lax.dot_general(a, b, (((0,), (0,)), ((), ())), preferred_element_type=F32)


def dot_split(x, matrix):
    high = x.astype(BF)
    low = (x - high.astype(F32)).astype(BF)
    return dot(high, matrix) + dot(low, matrix)


def iota(shape, dim):
    return lax.broadcasted_iota(jnp.int32, shape, dim)


def norm_groups(x):
    matrix = jnp.where(iota((128, 128), 0) // 64 == iota((128, 128), 1) // 64, 1.0 / 64, 0.0)
    matrix = matrix.astype(BF)
    centred = x - dot_split(x, matrix)
    spread = dot_split(centred * centred, matrix)
    return centred * lax.rsqrt(spread + 1e-05)


def both_halves(x, odd):
    turned = pltpu.roll(x, 64, axis=1)
    low = iota(x.shape, 1) < 64
    return jnp.where(low, turned, x) if odd else jnp.where(low, x, turned)


def send_kernel(rows_hbm, pair_hbm, weight_hbm, out_ref, rows_ref, pair_ref, weight_ref, sems):
    copies = [pltpu.make_async_copy(rows_hbm, rows_ref, sems.at[0]),
              pltpu.make_async_copy(pair_hbm, pair_ref, sems.at[1]),
              pltpu.make_async_copy(weight_hbm, weight_ref, sems.at[2])]
    for copy in copies:
        copy.start()
    for copy in copies[1:]:
        copy.wait()
    pair = pair_ref[...].astype(F32)
    pair = pair - jnp.mean(pair, axis=-1, keepdims=True)
    pair = pair * lax.rsqrt(jnp.mean(pair * pair, axis=-1, keepdims=True) + 1e-05)
    lane = iota((8, 128), 1)
    terms = jnp.zeros((8, 128), F32)
    for h in range(8):
        bias = jnp.sum(pair * weight_ref[h:h + 1, :], axis=-1, keepdims=True)
        for k in range(3):
            term = bias.astype(BF).astype(F32)
            bias = bias - term
            terms = jnp.where(lane == k * 8 + h, term, terms)
    terms = terms.astype(BF)
    for peer in range(8):
        out_ref[peer, 4] = terms
    copies[0].wait()
    for peer in range(8):
        low = rows_ref[peer * 8:peer * 8 + 4].astype(F32)
        high = rows_ref[peer * 8 + 4:peer * 8 + 8].astype(F32)
        out_ref[peer, 0:4] = jnp.concatenate([low, high], axis=-1).astype(BF)


def bias_kernel(count_ref, mask_ref, members_ref, all_ref, out_ref, scratch):
    terms = all_ref[:, 4].astype(F32).reshape(64, 128).T
    bias = terms[0:8] + terms[8:16] + terms[16:24]
    bias = bias + jnp.where(mask_ref[lax.axis_index("seq")] == 1, 0.0, -1000000.0)
    scratch[...] = jnp.concatenate([bias, bias], axis=1)
    for k in range(4):
        row = jnp.where(iota((1, 128), 1) < 64, scratch[2 * k:2 * k + 1, :],
                        scratch[2 * k + 1:2 * k + 2, :])
        out_ref[:, :, k * 128:(k + 1) * 128] = jnp.broadcast_to(row[None], (64, 1, 128))
    weight = jnp.where(iota((1, 64), 1) < count_ref[0], members_ref[...], 0).astype(F32)
    total = jnp.sum(weight, axis=1, keepdims=True)
    out_ref[:, :, 512:640] = jnp.broadcast_to(total[None], (64, 1, 128))


def project_kernel(all_ref, in_w_ref, outer_w_ref, raw_out, k_out, q_out, v_out, gate_out, w_out):
    raw = jnp.concatenate([all_ref[:, p].astype(F32).reshape(64, 128) for p in range(4)], axis=0)
    normed = norm_groups(raw).astype(BF)
    raw = raw.astype(BF)
    weight = in_w_ref[...]
    turned = weight.astype(F32).T
    turned = jnp.concatenate([turned[0:64], turned[128:256]], axis=0)
    zero = jnp.zeros_like(turned)
    key_w = weight[:, 64:128]
    key_zero = jnp.zeros_like(key_w)
    row, lane = iota((64, 128), 0), iota((64, 128), 1)
    for half in range(2):
        sides = [turned, zero] if half == 0 else [zero, turned]
        qvg = dot_nt(jnp.concatenate(sides, axis=1).astype(BF), normed)
        sides = [key_w, key_zero] if half == 0 else [key_zero, key_w]
        k_out[half] = dot(normed, jnp.concatenate(sides, axis=0)).astype(BF)
        pick = (lane == row + 64 * half).astype(BF)
        raw_out[:, half * 256:(half + 1) * 256] = dot_nt(pick, raw)
        gate_out[:, half * 256:(half + 1) * 256] = jax.nn.sigmoid(qvg[128:192])
        for place in range(4):
            e = half * 4 + place
            v_out[e] = qvg[64:128, place * 64:(place + 1) * 64].astype(BF)
            q = qvg[0:64, place // 2 * 128:(place // 2 + 1) * 128] * (1.0 / math.sqrt(8))
            q = both_halves(q, place % 2)
            for k in range(4):
                own = row // 8 == 2 * k + lane // 64
                q_out[e, :, k * 128:(k + 1) * 128] = jnp.where(own, q, 0.0).astype(BF)
    for c in range(32):
        w_out[c % 2, :, c // 2 * 32:(c // 2 + 1) * 32] = (
            outer_w_ref[c * 32:(c + 1) * 32, :].T.astype(BF))


def attend_kernel(count_ref, members_ref, mask_ref, bias_ref, raw_ref, k_ref, q_ref, v_ref,
                  gate_ref, out_w_ref, factor_ref, out_ref, left_scr, right_scr):
    bias = jnp.concatenate([bias_ref[pl.ds(k, 64, stride=5), :] for k in range(4)], axis=1)
    lane = iota((8, 128), 1)
    probs = []
    for e in range(8):
        keys = k_ref[e // 4, e % 4 * 64:(e % 4 + 1) * 64, :]
        scores = dot(keys, q_ref[e]) + bias
        expo = jnp.exp(scores - jnp.max(scores, axis=0, keepdims=True))
        probs.append((expo * (1.0 / jnp.sum(expo, axis=0, keepdims=True))).astype(BF))
    columns = []
    for pair in range(4):
        full = [dot(v_ref[2 * pair + odd], probs[2 * pair + odd]) for odd in range(2)]
        heads = []
        for h in range(8):
            low, high = [f[h * 8:(h + 1) * 8, h // 2 * 128:(h // 2 + 1) * 128] for f in full]
            if h % 2 == 0:
                high = pltpu.roll(high, 64, axis=1)
            else:
                low = pltpu.roll(low, 64, axis=1)
            heads.append(jnp.where(lane < 64, low, high))
        columns.append(jnp.concatenate(heads, axis=0))
    context = jnp.concatenate(columns, axis=1)
    gated = (gate_ref[...] * context).astype(BF)

    base = lax.axis_index("res") * 8
    keep = (mask_ref[...] == 1).astype(F32)
    keep = jnp.concatenate([keep, keep], axis=1)
    usable = [(base + e < count_ref[0]).astype(F32) for e in range(8)]
    weights = [members_ref[base + e].astype(F32) * usable[e] for e in range(8)]
    low = iota((1, 128), 1) < 64
    used = jnp.concatenate([jnp.where(low, usable[2 * p], usable[2 * p + 1]) for p in range(4)],
                           axis=1)
    scale = jnp.concatenate([jnp.where(low, weights[2 * p], weights[2 * p + 1]) * keep
                             for p in range(4)], axis=1)

    out_w = out_w_ref[...]
    x = raw_ref[...] + dot_tn(out_w, gated).astype(BF).astype(F32) * used
    x = x - jnp.mean(x, axis=0, keepdims=True)
    x = (x * lax.rsqrt(jnp.mean(x * x, axis=0, keepdims=True) + 1e-05)).astype(BF)
    factor = factor_ref[...]

    left = dot_tn(factor[:, 0:32], x) * scale
    for e in range(8):
        both = left[:, e // 2 * 128:(e // 2 + 1) * 128]
        left_scr[e * 32:(e + 1) * 32, :] = both_halves(both, e % 2)
    for c in range(16):
        block = jnp.where(lane < 64, left_scr[pl.ds(2 * c, 8, stride=32), :],
                          left_scr[pl.ds(2 * c + 1, 8, stride=32), :]).astype(BF)
        for peer in range(8):
            out_ref[peer, c] = block

    update = dot_tn(gated, jnp.concatenate([out_w, out_w], axis=1))
    for place in range(4):
        first = jnp.where(iota((64, 128), 1) < 64,
                          update[place * 64:(place + 1) * 64] * usable[place],
                          update[(place + 4) * 64:(place + 5) * 64] * usable[place + 4])
        first = first.reshape(8, 8, 128).astype(BF)
        for peer in range(8):
            out_ref[peer, 16 + place] = first[peer]

    right_w = jnp.concatenate([factor[:, 32:64]] * 4, axis=1)
    right_scr[...] = dot_tn(x, right_w)
    for peer in range(8):
        for quad in range(2):
            first = peer * 8 + quad * 4
            a, b, c, d = [right_scr[pl.ds(first + j, 8, stride=64), :] for j in range(4)]
            block = jnp.where(lane < 64, jnp.where(lane < 32, a, b), jnp.where(lane < 96, c, d))
            out_ref[peer, 20 + quad] = block.astype(BF)


def outer_kernel(mask_ref, all_ref, weight_ref, out_ref, part_scr):
    def gathered(block):
        return all_ref[:, block].astype(F32).reshape(64, 128)

    base = lax.axis_index("res") * 8
    lane = iota((1, 128), 1)
    right = []
    for quad in range(2):
        keep = jnp.zeros((1, 128), F32)
        for j in range(4):
            mine = (mask_ref[base + quad * 4 + j] == 1).astype(F32)
            keep = jnp.where(lane // 32 == j, mine, keep)
        right.append((gathered(20 + quad) * keep).astype(BF))
    right = jnp.concatenate(right, axis=1)
    left = jnp.concatenate([gathered(c).astype(BF) for c in range(16)], axis=1)
    outer = dot_tn(right, left).astype(BF)
    pick = (iota((64, 128), 0) == iota((64, 128), 1)).astype(BF)
    for j in range(8):
        rows = outer[j * 32:(j + 1) * 32]
        stacked = jnp.concatenate([rows[:, c * 128:(c + 1) * 128] for c in range(16)], axis=0)
        even, odd = dot(weight_ref[0], stacked), dot(weight_ref[1], stacked)
        part = (even + pltpu.roll(odd, 64, axis=1)).astype(BF)
        part_scr[pl.ds(j, 64, stride=8), :] = dot_nt(pick, part)
    out_ref[...] = part_scr[...].reshape(64, 8, 128).astype(BF)


def update_kernel(all_ref, out_ref):
    for place in range(4):
        block = all_ref[:, 16 + place].astype(F32)
        for half in range(2):
            part = block[:, :, half * 64:(half + 1) * 64].astype(BF)
            for peer in range(8):
                out_ref[peer * 8 + half * 4 + place] = part[peer]


def call(kernel, outs, specs, scratch=(), flops=0, limit=8):
    return pl.pallas_call(
        kernel,
        out_shape=[jax.ShapeDtypeStruct(shape, kind) for shape, kind in outs],
        in_specs=specs,
        out_specs=[VMEM] * len(outs),
        scratch_shapes=[s if not isinstance(s, tuple) else pltpu.VMEM(*s) for s in scratch],
        cost_estimate=pl.CostEstimate(flops=flops, bytes_accessed=1 << 20, transcendentals=0),
        compiler_params=pltpu.CompilerParams(vmem_limit_bytes=limit << 20),
    )


def local(
    alignment_rows,
    pair_features,
    sequence_block_count,
    cluster_member_count,
    residue_present_mask,
    attention_in_weight,
    attention_out_weight,
    pair_bias_weight,
    outer_factor_weight,
    outer_output_weight,
    outer_product_bias,
):
    (send,) = call(
        send_kernel, [((8, 5, 8, 128), BF)], [HBM] * 3,
        [((64, 8, 64), BF), ((8, 128), BF), ((8, 128), F32), pltpu.SemaphoreType.DMA((3,))],
    )(alignment_rows, pair_features.reshape(8, 128), pair_bias_weight.T)
    rows_all = lax.all_to_all(send, "res", split_axis=0, concat_axis=0, tiled=True)
    (bias_send,) = call(
        bias_kernel, [((64, 1, 640), F32)], [SMEM] * 2 + [VMEM] * 2, [((8, 128), F32)],
    )(sequence_block_count, residue_present_mask, cluster_member_count.reshape(1, 64), rows_all)
    bias_all = lax.all_to_all(bias_send, "seq", split_axis=0, concat_axis=0, tiled=True)
    bias_all = bias_all.reshape(320, 128)
    raw, keys, queries, values, gate, outer_w = call(
        project_kernel,
        [((64, 512), F32), ((2, 256, 64), BF), ((8, 64, 512), BF), ((8, 64, 64), BF),
         ((64, 512), F32), ((2, 128, 512), BF)],
        [VMEM] * 3,
        flops=1 << 30,
    )(rows_all, attention_in_weight, outer_output_weight)
    (factor_send,) = call(
        attend_kernel, [((8, 22, 8, 128), BF)], [SMEM] * 2 + [VMEM] * 9,
        [((256, 128), F32), ((512, 128), F32)],
    )(sequence_block_count, cluster_member_count, residue_present_mask.reshape(1, 64), bias_all,
      raw, keys, queries, values, gate, attention_out_weight, outer_factor_weight)
    factor_all = lax.all_to_all(factor_send, "res", split_axis=0, concat_axis=0, tiled=True)
    (partial,) = call(
        outer_kernel, [((64, 8, 128), BF)], [SMEM] + [VMEM] * 2, [((512, 128), F32)],
    )(residue_present_mask, factor_all, outer_w)
    arrived = lax.all_to_all(partial, "seq", split_axis=0, concat_axis=0, tiled=True)
    (row_attention_update,) = call(
        update_kernel, [((64, 8, 64), BF)], [VMEM], flops=1 << 30,
    )(factor_all)
    summed = arrived.astype(F32).sum(axis=0)
    weight_sum = jnp.sum(bias_all.reshape(64, 640)[:, 512])
    pair_update = (summed / weight_sum + outer_product_bias).astype(BF)
    return (row_attention_update, pair_update[None])


def solution(mesh):
    return jax.shard_map(
        local,
        mesh=mesh,
        in_specs=(
            P("seq", "res", None),
            P("res", "seq", None),
            P("seq"),
            P("seq"),
            P(),
            P(),
            P(),
            P(),
            P(),
            P(),
            P(),
        ),
        out_specs=(P("seq", "res", None), P("seq", "res", None)),
        check_vma=False,
    )
```

```python
import math

import jax
import jax.numpy as jnp
from jax import lax
from jax.experimental import pallas as pl
from jax.experimental.pallas import tpu as pltpu
from jax.sharding import PartitionSpec as P

BF = jnp.bfloat16
F32 = jnp.float32
VMEM = pl.BlockSpec(memory_space=pltpu.VMEM)
SMEM = pl.BlockSpec(memory_space=pltpu.SMEM)
HBM = pl.BlockSpec(memory_space=pltpu.HBM)


def dot(a, b):
    return jnp.dot(a, b, preferred_element_type=F32)


def dot_nt(a, b):
    return lax.dot_general(a, b, (((1,), (1,)), ((), ())), preferred_element_type=F32)


def dot_tn(a, b):
    return lax.dot_general(a, b, (((0,), (0,)), ((), ())), preferred_element_type=F32)


def dot_split(x, matrix):
    high = x.astype(BF)
    low = (x - high.astype(F32)).astype(BF)
    return dot(high, matrix) + dot(low, matrix)


def iota(shape, dim):
    return lax.broadcasted_iota(jnp.int32, shape, dim)


def norm_groups(x):
    matrix = jnp.where(iota((128, 128), 0) // 64 == iota((128, 128), 1) // 64, 1.0 / 64, 0.0)
    matrix = matrix.astype(BF)
    centred = x - dot_split(x, matrix)
    spread = dot_split(centred * centred, matrix)
    return centred * lax.rsqrt(spread + 1e-05)


def both_halves(x, odd):
    turned = pltpu.roll(x, 64, axis=1)
    low = iota(x.shape, 1) < 64
    return jnp.where(low, turned, x) if odd else jnp.where(low, x, turned)


def bias_kernel(pair_hbm, weight_hbm, members_hbm, count_hbm, out_ref,
                pair_ref, weight_ref, members_ref, count_ref, sems):
    copies = [pltpu.make_async_copy(pair_hbm, pair_ref, sems.at[0]),
              pltpu.make_async_copy(weight_hbm, weight_ref, sems.at[1]),
              pltpu.make_async_copy(members_hbm, members_ref, sems.at[2]),
              pltpu.make_async_copy(count_hbm, count_ref, sems.at[3])]
    for copy in copies:
        copy.start()
    for copy in copies:
        copy.wait()
    pair = pair_ref[...].astype(F32)
    pair = pair - jnp.mean(pair, axis=-1, keepdims=True)
    pair = pair * lax.rsqrt(jnp.mean(pair * pair, axis=-1, keepdims=True) + 1e-05)
    row, lane = iota((8, 128), 0), iota((8, 128), 1)
    bias = jnp.zeros((8, 128), F32)
    for h in range(8):
        column = jnp.sum(pair * weight_ref[h:h + 1, :], axis=-1, keepdims=True)
        bias = jnp.where(lane == h * 8 + row, column, bias)
    bias = jnp.sum(bias, axis=0, keepdims=True)
    weight = jnp.where(iota((1, 64), 1) < count_ref[...], members_ref[...], 0).astype(F32)
    bias = jnp.where(lane[0:1] < 64, bias, jnp.sum(weight, axis=1, keepdims=True))
    out_ref[...] = jnp.broadcast_to(bias[None], (64, 1, 128))


def pack_kernel(rows_ref, out_ref):
    for peer in range(8):
        low = rows_ref[peer * 8:peer * 8 + 4].astype(F32)
        high = rows_ref[peer * 8 + 4:peer * 8 + 8].astype(F32)
        out_ref[peer] = jnp.concatenate([low, high], axis=-1).astype(BF)


def send_kernel(rows_ref, bias_ref, out_ref):
    for peer in range(8):
        out_ref[peer, 0:4] = rows_ref[peer]
    bias = bias_ref[...]
    high = bias.astype(BF).astype(F32)
    terms = jnp.where(iota((64, 128), 1) < 64, high, pltpu.roll(bias - high, 64, axis=1))
    terms = terms.reshape(8, 8, 128).astype(BF)
    for peer in range(8):
        out_ref[peer, 4:12] = terms


def weight_kernel(outer_w_ref, w_out, place_out):
    for c in range(32):
        w_out[c % 2, :, c // 2 * 32:(c // 2 + 1) * 32] = (
            outer_w_ref[c * 32:(c + 1) * 32, :].T.astype(BF))
    for peer in range(8):
        row, lane = iota((128, 512), 0), iota((128, 512), 1)
        target = row % 64 // 8 * 64 + peer * 8 + row % 8
        place_out[peer * 128:(peer + 1) * 128, :] = (lane == target).astype(BF)


def project(all_ref, in_w_ref, raw_out, k_out, q_out, v_out, gate_out):
    raw = jnp.concatenate([all_ref[:, p].astype(F32).reshape(64, 128) for p in range(4)], axis=0)
    normed = norm_groups(raw).astype(BF)
    raw = raw.astype(BF)
    weight = in_w_ref[...]
    turned = weight.astype(F32).T
    turned = jnp.concatenate([turned[0:64], turned[128:256]], axis=0)
    zero = jnp.zeros_like(turned)
    key_w = weight[:, 64:128]
    key_zero = jnp.zeros_like(key_w)
    row, lane = iota((64, 128), 0), iota((64, 128), 1)
    for half in range(2):
        sides = [turned, zero] if half == 0 else [zero, turned]
        qvg = dot_nt(jnp.concatenate(sides, axis=1).astype(BF), normed)
        sides = [key_w, key_zero] if half == 0 else [key_zero, key_w]
        k_out[half] = dot(normed, jnp.concatenate(sides, axis=0)).astype(BF)
        pick = (lane == row + 64 * half).astype(BF)
        raw_out[:, half * 256:(half + 1) * 256] = dot_nt(pick, raw)
        gate_out[:, half * 256:(half + 1) * 256] = jax.nn.sigmoid(qvg[128:192])
        for place in range(4):
            e = half * 4 + place
            v_out[e] = qvg[64:128, place * 64:(place + 1) * 64].astype(BF)
            q = qvg[0:64, place // 2 * 128:(place // 2 + 1) * 128] * (1.0 / math.sqrt(8))
            q = both_halves(q, place % 2)
            for k in range(4):
                own = row // 8 == 2 * k + lane // 64
                q_out[e, :, k * 128:(k + 1) * 128] = jnp.where(own, q, 0.0).astype(BF)


def attend_kernel(members_ref, count_ref, mask_ref, all_ref, place_ref, in_w_ref, out_w_ref,
                  factor_ref, out_ref, raw_ref, k_ref, q_ref, v_ref, gate_ref, left_scr,
                  right_scr):
    project(all_ref, in_w_ref, raw_ref, k_ref, q_ref, v_ref, gate_ref)
    terms = [all_ref[peer, 4:12].astype(F32).reshape(64, 128).astype(BF) for peer in range(8)]
    present = jnp.where(iota((64, 64), 0) == iota((64, 64), 1), mask_ref[...], 0)
    present = jnp.sum(present.astype(F32), axis=1, keepdims=True)
    bias = dot(jnp.concatenate(terms, axis=1), place_ref[...])
    bias = bias + jnp.where(present == 1.0, 0.0, -1000000.0)
    lane = iota((8, 128), 1)
    probs = []
    for e in range(8):
        keys = k_ref[e // 4, e % 4 * 64:(e % 4 + 1) * 64, :]
        scores = dot(keys, q_ref[e]) + bias
        expo = jnp.exp(scores - jnp.max(scores, axis=0, keepdims=True))
        probs.append((expo * (1.0 / jnp.sum(expo, axis=0, keepdims=True))).astype(BF))
    columns = []
    for pair in range(4):
        full = [dot(v_ref[2 * pair + odd], probs[2 * pair + odd]) for odd in range(2)]
        heads = []
        for h in range(8):
            low, high = [f[h * 8:(h + 1) * 8, h // 2 * 128:(h // 2 + 1) * 128] for f in full]
            if h % 2 == 0:
                high = pltpu.roll(high, 64, axis=1)
            else:
                low = pltpu.roll(low, 64, axis=1)
            heads.append(jnp.where(lane < 64, low, high))
        columns.append(jnp.concatenate(heads, axis=0))
    context = jnp.concatenate(columns, axis=1)
    gated = (gate_ref[...] * context).astype(BF)

    base = lax.axis_index("res") * 8
    keep = (mask_ref[...] == 1).astype(F32)
    keep = jnp.concatenate([keep, keep], axis=1)
    usable = [(base + e < count_ref[...]).astype(F32) for e in range(8)]
    weights = [members_ref[base + e].astype(F32) * usable[e] for e in range(8)]
    low = iota((1, 128), 1) < 64
    used = jnp.concatenate([jnp.where(low, usable[2 * p], usable[2 * p + 1]) for p in range(4)],
                           axis=1)
    scale = jnp.concatenate([jnp.where(low, weights[2 * p], weights[2 * p + 1]) * keep
                             for p in range(4)], axis=1)

    out_w = out_w_ref[...]
    x = raw_ref[...] + dot_tn(out_w, gated).astype(BF).astype(F32) * used
    x = x - jnp.mean(x, axis=0, keepdims=True)
    x = (x * lax.rsqrt(jnp.mean(x * x, axis=0, keepdims=True) + 1e-05)).astype(BF)
    factor = factor_ref[...]

    left = dot_tn(factor[:, 0:32], x) * scale
    for e in range(8):
        both = left[:, e // 2 * 128:(e // 2 + 1) * 128]
        left_scr[e * 32:(e + 1) * 32, :] = both_halves(both, e % 2)
    for c in range(16):
        block = jnp.where(lane < 64, left_scr[pl.ds(2 * c, 8, stride=32), :],
                          left_scr[pl.ds(2 * c + 1, 8, stride=32), :]).astype(BF)
        for peer in range(8):
            out_ref[peer, c] = block

    update = dot_tn(gated, jnp.concatenate([out_w, out_w], axis=1))
    for place in range(4):
        first = jnp.where(iota((64, 128), 1) < 64,
                          update[place * 64:(place + 1) * 64] * usable[place],
                          update[(place + 4) * 64:(place + 5) * 64] * usable[place + 4])
        first = first.reshape(8, 8, 128).astype(BF)
        for peer in range(8):
            out_ref[peer, 16 + place] = first[peer]

    right_w = jnp.concatenate([factor[:, 32:64]] * 4, axis=1)
    right_scr[...] = dot_tn(x, right_w)
    for peer in range(8):
        for quad in range(2):
            first = peer * 8 + quad * 4
            a, b, c, d = [right_scr[pl.ds(first + j, 8, stride=64), :] for j in range(4)]
            block = jnp.where(lane < 64, jnp.where(lane < 32, a, b), jnp.where(lane < 96, c, d))
            out_ref[peer, 20 + quad] = block.astype(BF)


def outer_kernel(mask_ref, all_ref, weight_ref, out_ref, part_scr):
    def gathered(block):
        return all_ref[:, block].astype(F32).reshape(64, 128)

    base = lax.axis_index("res") * 8
    lane = iota((1, 128), 1)
    right = []
    for quad in range(2):
        keep = jnp.zeros((1, 128), F32)
        for j in range(4):
            mine = (mask_ref[base + quad * 4 + j] == 1).astype(F32)
            keep = jnp.where(lane // 32 == j, mine, keep)
        right.append((gathered(20 + quad) * keep).astype(BF))
    right = jnp.concatenate(right, axis=1)
    left = jnp.concatenate([gathered(c).astype(BF) for c in range(16)], axis=1)
    outer = dot_tn(right, left).astype(BF)
    pick = (iota((64, 128), 0) == iota((64, 128), 1)).astype(BF)
    for j in range(8):
        rows = outer[j * 32:(j + 1) * 32]
        stacked = jnp.concatenate([rows[:, c * 128:(c + 1) * 128] for c in range(16)], axis=0)
        even, odd = dot(weight_ref[0], stacked), dot(weight_ref[1], stacked)
        part = (even + pltpu.roll(odd, 64, axis=1)).astype(BF)
        part_scr[pl.ds(j, 64, stride=8), :] = dot_nt(pick, part)
    out_ref[...] = part_scr[...].reshape(64, 8, 128).astype(BF)


def update_kernel(all_ref, out_ref):
    for place in range(4):
        block = all_ref[:, 16 + place].astype(F32)
        for half in range(2):
            part = block[:, :, half * 64:(half + 1) * 64].astype(BF)
            for peer in range(8):
                out_ref[peer * 8 + half * 4 + place] = part[peer]


def call(kernel, outs, specs, scratch=(), flops=0, limit=8):
    return pl.pallas_call(
        kernel,
        out_shape=[jax.ShapeDtypeStruct(shape, kind) for shape, kind in outs],
        in_specs=specs,
        out_specs=[VMEM] * len(outs),
        scratch_shapes=[s if not isinstance(s, tuple) else pltpu.VMEM(*s) for s in scratch],
        cost_estimate=pl.CostEstimate(flops=flops, bytes_accessed=1 << 20, transcendentals=0),
        compiler_params=pltpu.CompilerParams(vmem_limit_bytes=limit << 20),
    )


def local(
    alignment_rows,
    pair_features,
    sequence_block_count,
    cluster_member_count,
    residue_present_mask,
    attention_in_weight,
    attention_out_weight,
    pair_bias_weight,
    outer_factor_weight,
    outer_output_weight,
    outer_product_bias,
):
    members = cluster_member_count.reshape(1, 64)
    count = sequence_block_count.reshape(1, 1)
    (packed,) = call(
        pack_kernel, [((8, 4, 8, 128), BF)], [VMEM], flops=1 << 30,
    )(alignment_rows)
    (bias_send,) = call(
        bias_kernel, [((64, 1, 128), F32)], [HBM] * 4,
        [((8, 128), BF), ((8, 128), F32), ((1, 64), jnp.int32), ((1, 1), jnp.int32),
         pltpu.SemaphoreType.DMA((4,))],
        limit=60,
    )(pair_features.reshape(8, 128), pair_bias_weight.T, members, count)
    bias_all = lax.all_to_all(bias_send, "seq", split_axis=0, concat_axis=0, tiled=True)
    bias_all = bias_all.reshape(64, 128)
    outer_w, place = call(
        weight_kernel, [((2, 128, 512), BF), ((1024, 512), BF)], [VMEM], flops=1 << 30,
    )(outer_output_weight)
    (send,) = call(
        send_kernel, [((8, 12, 8, 128), BF)], [VMEM] * 2,
    )(packed, bias_all)
    rows_all = lax.all_to_all(send, "res", split_axis=0, concat_axis=0, tiled=True)
    (factor_send,) = call(
        attend_kernel, [((8, 22, 8, 128), BF)], [SMEM] + [VMEM] * 7,
        [((64, 512), F32), ((2, 256, 64), BF), ((8, 64, 512), BF), ((8, 64, 64), BF),
         ((64, 512), F32), ((256, 128), F32), ((512, 128), F32)],
    )(cluster_member_count, count, residue_present_mask.reshape(1, 64), rows_all, place,
      attention_in_weight, attention_out_weight, outer_factor_weight)
    factor_all = lax.all_to_all(factor_send, "res", split_axis=0, concat_axis=0, tiled=True)
    (partial,) = call(
        outer_kernel, [((64, 8, 128), BF)], [SMEM] + [VMEM] * 2, [((512, 128), F32)],
    )(residue_present_mask, factor_all, outer_w)
    arrived = lax.all_to_all(partial, "seq", split_axis=0, concat_axis=0, tiled=True)
    (row_attention_update,) = call(
        update_kernel, [((64, 8, 64), BF)], [VMEM], flops=1 << 30,
    )(factor_all)
    summed = arrived.astype(F32).sum(axis=0)
    weight_sum = jnp.sum(bias_all[:, 64])
    pair_update = (summed / weight_sum + outer_product_bias).astype(BF)
    return (row_attention_update, pair_update[None])


def solution(mesh):
    return jax.shard_map(
        local,
        mesh=mesh,
        in_specs=(
            P("seq", "res", None),
            P("res", "seq", None),
            P("seq"),
            P("seq"),
            P(),
            P(),
            P(),
            P(),
            P(),
            P(),
            P(),
        ),
        out_specs=(P("seq", "res", None), P("seq", "res", None)),
        check_vma=False,
    )
```

```python
import math

import jax
import jax.numpy as jnp
from jax import lax
from jax.experimental import pallas as pl
from jax.experimental.pallas import tpu as pltpu
from jax.sharding import PartitionSpec as P

BF = jnp.bfloat16
F32 = jnp.float32
VMEM = pl.BlockSpec(memory_space=pltpu.VMEM)
SMEM = pl.BlockSpec(memory_space=pltpu.SMEM)
HBM = pl.BlockSpec(memory_space=pltpu.HBM)


def dot(a, b):
    return jnp.dot(a, b, preferred_element_type=F32)


def dot_nt(a, b):
    return lax.dot_general(a, b, (((1,), (1,)), ((), ())), preferred_element_type=F32)


def dot_tn(a, b):
    return lax.dot_general(a, b, (((0,), (0,)), ((), ())), preferred_element_type=F32)


def dot_split(x, matrix):
    high = x.astype(BF)
    low = (x - high.astype(F32)).astype(BF)
    return dot(high, matrix) + dot(low, matrix)


def iota(shape, dim):
    return lax.broadcasted_iota(jnp.int32, shape, dim)


def norm_groups(x):
    matrix = jnp.where(iota((128, 128), 0) // 64 == iota((128, 128), 1) // 64, 1.0 / 64, 0.0)
    matrix = matrix.astype(BF)
    centred = x - dot_split(x, matrix)
    spread = dot_split(centred * centred, matrix)
    return centred * lax.rsqrt(spread + 1e-05)


def both_halves(x, odd):
    turned = pltpu.roll(x, 64, axis=1)
    low = iota(x.shape, 1) < 64
    return jnp.where(low, turned, x) if odd else jnp.where(low, x, turned)


def bias_kernel(pair_hbm, weight_hbm, members_hbm, count_hbm, out_ref,
                pair_ref, weight_ref, members_ref, count_ref, sems):
    copies = [pltpu.make_async_copy(pair_hbm, pair_ref, sems.at[0]),
              pltpu.make_async_copy(weight_hbm, weight_ref, sems.at[1]),
              pltpu.make_async_copy(members_hbm, members_ref, sems.at[2]),
              pltpu.make_async_copy(count_hbm, count_ref, sems.at[3])]
    for copy in copies:
        copy.start()
    for copy in copies:
        copy.wait()
    pair = pair_ref[...].astype(F32)
    pair = pair - jnp.mean(pair, axis=-1, keepdims=True)
    pair = pair * lax.rsqrt(jnp.mean(pair * pair, axis=-1, keepdims=True) + 1e-05)
    row, lane = iota((8, 128), 0), iota((8, 128), 1)
    bias = jnp.zeros((8, 128), F32)
    for h in range(8):
        column = jnp.sum(pair * weight_ref[h:h + 1, :], axis=-1, keepdims=True)
        bias = jnp.where(lane == h * 8 + row, column, bias)
    bias = jnp.sum(bias, axis=0, keepdims=True)
    weight = jnp.where(iota((1, 64), 1) < count_ref[0], members_ref[...], 0).astype(F32)
    bias = jnp.where(lane[0:1] < 64, bias, jnp.sum(weight, axis=1, keepdims=True))
    out_ref[...] = jnp.broadcast_to(bias[None], (64, 1, 128))


def pack_kernel(rows_ref, out_ref):
    for peer in range(8):
        low = rows_ref[peer * 8:peer * 8 + 4].astype(F32)
        high = rows_ref[peer * 8 + 4:peer * 8 + 8].astype(F32)
        out_ref[peer] = jnp.concatenate([low, high], axis=-1).astype(BF)


def send_kernel(rows_ref, bias_ref, ahead_ref, out_ref, inverse_out):
    for peer in range(8):
        out_ref[peer, 0:4] = rows_ref[peer]
    bias = bias_ref[...]
    lane = iota((64, 128), 1)
    high = bias.astype(BF).astype(F32)
    terms = jnp.where(lane < 64, high, pltpu.roll(bias - high, 64, axis=1))
    terms = terms.reshape(8, 8, 128).astype(BF)
    for peer in range(8):
        out_ref[peer, 4:12] = terms
    total = jnp.sum(bias, axis=0, keepdims=True)
    total = jnp.sum(jnp.where(lane[0:1] == 64, total, 0.0), axis=1, keepdims=True)
    inverse_out[...] = jnp.broadcast_to(1.0 / total, (8, 128))


def weight_kernel(outer_w_ref, in_w_ref, out_w_ref, factor_ref, shift_ref, members_ref, mask_ref,
                  count_ref, w_out, place_out, qvg_out, key_out, wide_out, left_out, right_out,
                  shift_out, used_out, scale_out, absent_out, keep_out):
    w_out[...] = outer_w_ref[...].astype(BF)
    for peer in range(8):
        row, lane = iota((128, 512), 0), iota((128, 512), 1)
        target = row % 64 // 8 * 64 + peer * 8 + row % 8
        place_out[peer * 128:(peer + 1) * 128, :] = (lane == target).astype(BF)
    weight = in_w_ref[...]
    turned = weight.astype(F32).T
    turned = jnp.concatenate([turned[0:64], turned[128:256]], axis=0)
    zero = jnp.zeros_like(turned)
    qvg_out[0] = jnp.concatenate([turned, zero], axis=1).astype(BF)
    qvg_out[1] = jnp.concatenate([zero, turned], axis=1).astype(BF)
    key_w = weight[:, 64:128]
    zero = jnp.zeros_like(key_w)
    key_out[0] = jnp.concatenate([key_w, zero], axis=0)
    key_out[1] = jnp.concatenate([zero, key_w], axis=0)
    out_w = out_w_ref[...]
    wide_out[...] = jnp.concatenate([out_w, out_w], axis=1)
    factor = factor_ref[...]
    left_out[...] = factor[:, 0:32]
    right_out[...] = jnp.concatenate([factor[:, 32:64]] * 4, axis=1)
    shift_out[...] = jnp.broadcast_to(shift_ref[...], (8, 128))
    base = lax.axis_index("res") * 8
    count = count_ref[...]
    members = jnp.where(iota((1, 64), 1) < count, members_ref[...], 0).astype(F32)
    present = (mask_ref[...] == 1).astype(F32)
    mine = (iota((64, 512), 0) == base + iota((64, 512), 1) // 64).astype(BF)
    scale = dot(members.astype(BF), mine)
    scale_out[...] = scale * jnp.concatenate([present] * 8, axis=1)
    used_out[...] = (base + iota((1, 512), 1) // 64 < count).astype(F32)
    mine = (iota((64, 256), 0) == base + iota((64, 256), 1) // 32).astype(BF)
    keep_out[...] = dot(present.astype(BF), mine)
    column = jnp.where(iota((64, 64), 0) == iota((64, 64), 1), present, 0.0)
    column = jnp.sum(column, axis=1, keepdims=True)
    absent_out[...] = jnp.broadcast_to(jnp.where(column == 1.0, 0.0, -1000000.0), (64, 128))


def project(all_ref, qvg_ref, key_ref, raw_out, k_out, q_out, v_out, gate_out):
    raw = jnp.concatenate([all_ref[:, p].astype(F32).reshape(64, 128) for p in range(4)], axis=0)
    normed = norm_groups(raw).astype(BF)
    raw = raw.astype(BF)
    row, lane = iota((64, 128), 0), iota((64, 128), 1)
    for half in range(2):
        qvg = dot_nt(qvg_ref[half], normed)
        k_out[half] = dot(normed, key_ref[half]).astype(BF)
        pick = (lane == row + 64 * half).astype(BF)
        raw_out[:, half * 256:(half + 1) * 256] = dot_nt(pick, raw)
        gate_out[:, half * 256:(half + 1) * 256] = jax.nn.sigmoid(qvg[128:192])
        for place in range(4):
            e = half * 4 + place
            v_out[e] = qvg[64:128, place * 64:(place + 1) * 64].astype(BF)
            q = qvg[0:64, place // 2 * 128:(place // 2 + 1) * 128] * (1.0 / math.sqrt(8))
            q = both_halves(q, place % 2)
            for k in range(4):
                own = row // 8 == 2 * k + lane // 64
                q_out[e, :, k * 128:(k + 1) * 128] = jnp.where(own, q, 0.0).astype(BF)


def attend_kernel(all_ref, place_ref, qvg_ref, key_ref, wide_ref, left_ref, right_ref, used_ref,
                  scale_ref, absent_ref, out_ref, raw_ref, k_ref, q_ref, v_ref, gate_ref,
                  left_scr, right_scr):
    project(all_ref, qvg_ref, key_ref, raw_ref, k_ref, q_ref, v_ref, gate_ref)
    terms = [all_ref[peer, 4:12].astype(F32).reshape(64, 128).astype(BF) for peer in range(8)]
    bias = dot(jnp.concatenate(terms, axis=1), place_ref[...])
    bias = bias + jnp.concatenate([absent_ref[...]] * 4, axis=1)
    lane = iota((8, 128), 1)
    probs = []
    for e in range(8):
        keys = k_ref[e // 4, e % 4 * 64:(e % 4 + 1) * 64, :]
        scores = dot(keys, q_ref[e]) + bias
        expo = jnp.exp(scores - jnp.max(scores, axis=0, keepdims=True))
        probs.append((expo * (1.0 / jnp.sum(expo, axis=0, keepdims=True))).astype(BF))
    columns = []
    for pair in range(4):
        full = [dot(v_ref[2 * pair + odd], probs[2 * pair + odd]) for odd in range(2)]
        heads = []
        for h in range(8):
            low, high = [f[h * 8:(h + 1) * 8, h // 2 * 128:(h // 2 + 1) * 128] for f in full]
            if h % 2 == 0:
                high = pltpu.roll(high, 64, axis=1)
            else:
                low = pltpu.roll(low, 64, axis=1)
            heads.append(jnp.where(lane < 64, low, high))
        columns.append(jnp.concatenate(heads, axis=0))
    context = jnp.concatenate(columns, axis=1)
    gated = (gate_ref[...] * context).astype(BF)

    used = used_ref[...]
    wide = wide_ref[...]
    x = raw_ref[...] + dot_tn(wide[:, 0:64], gated).astype(BF).astype(F32) * used
    x = x - jnp.mean(x, axis=0, keepdims=True)
    x = (x * lax.rsqrt(jnp.mean(x * x, axis=0, keepdims=True) + 1e-05)).astype(BF)

    left = dot_tn(left_ref[...], x) * scale_ref[...]
    for e in range(8):
        both = left[:, e // 2 * 128:(e // 2 + 1) * 128]
        left_scr[e * 32:(e + 1) * 32, :] = both_halves(both, e % 2)
    for c in range(16):
        block = jnp.where(lane < 64, left_scr[pl.ds(2 * c, 8, stride=32), :],
                          left_scr[pl.ds(2 * c + 1, 8, stride=32), :]).astype(BF)
        for peer in range(8):
            out_ref[peer, c] = block

    update = dot_tn(gated, wide)
    for place in range(4):
        low, high = [e * 64 for e in (place, place + 4)]
        first = jnp.where(iota((64, 128), 1) < 64,
                          update[low:low + 64] * used[:, low:low + 1],
                          update[high:high + 64] * used[:, high:high + 1])
        first = first.reshape(8, 8, 128).astype(BF)
        for peer in range(8):
            out_ref[peer, 16 + place] = first[peer]

    right_scr[...] = dot_tn(x, right_ref[...])
    for peer in range(8):
        for quad in range(2):
            first = peer * 8 + quad * 4
            a, b, c, d = [right_scr[pl.ds(first + j, 8, stride=64), :] for j in range(4)]
            block = jnp.where(lane < 64, jnp.where(lane < 32, a, b), jnp.where(lane < 96, c, d))
            out_ref[peer, 20 + quad] = block.astype(BF)


def outer_kernel(keep_ref, all_ref, weight_ref, out_ref, outer_scr, part_scr):
    def gathered(block):
        return all_ref[:, block].astype(F32).reshape(64, 128)

    right = jnp.concatenate([gathered(20), gathered(21)], axis=1) * keep_ref[...]
    right = right.astype(BF)
    lane = iota((64, 128), 1)
    for m in range(8):
        left = [gathered(c).astype(BF) for c in (2 * m, 2 * m + 1)]
        outer = dot_tn(jnp.concatenate(left, axis=1), right)
        for quad in range(2):
            pieces = [outer[k * 64:(k + 1) * 64, quad * 128:(quad + 1) * 128] for k in range(4)]
            for j in range(4):
                turned = [pltpu.roll(p, (k - j) * 32 % 128, axis=1) if k != j else p
                          for k, p in enumerate(pieces)]
                low = jnp.where(lane < 32, turned[0], turned[1])
                high = jnp.where(lane < 96, turned[2], turned[3])
                row = (quad * 4 + j) * 64
                outer_scr[row:row + 64, m * 128:(m + 1) * 128] = (
                    jnp.where(lane < 64, low, high).astype(BF))
    part = dot(outer_scr[...], weight_ref[...])
    for j in range(8):
        part_scr[pl.ds(j, 64, stride=8), :] = part[j * 64:(j + 1) * 64]
    out_ref[...] = part_scr[...].reshape(64, 8, 128).astype(BF)


def finish_kernel(arrived_ref, all_ref, inverse_ref, shift_ref, update_out, pair_out):
    for place in range(4):
        block = all_ref[:, 16 + place].astype(F32)
        for half in range(2):
            part = block[:, :, half * 64:(half + 1) * 64].astype(BF)
            for peer in range(8):
                update_out[peer * 8 + half * 4 + place] = part[peer]
    total = jnp.sum(arrived_ref[...].astype(F32), axis=0)
    pair_out[0] = (total * inverse_ref[...] + shift_ref[...]).astype(BF)


def call(kernel, outs, specs, scratch=(), flops=0, limit=8):
    return pl.pallas_call(
        kernel,
        out_shape=[jax.ShapeDtypeStruct(shape, kind) for shape, kind in outs],
        in_specs=specs,
        out_specs=[VMEM] * len(outs),
        scratch_shapes=[s if not isinstance(s, tuple) else pltpu.VMEM(*s) for s in scratch],
        cost_estimate=pl.CostEstimate(flops=flops, bytes_accessed=1 << 20, transcendentals=0),
        compiler_params=pltpu.CompilerParams(vmem_limit_bytes=limit << 20),
    )


def local(
    alignment_rows,
    pair_features,
    sequence_block_count,
    cluster_member_count,
    residue_present_mask,
    attention_in_weight,
    attention_out_weight,
    pair_bias_weight,
    outer_factor_weight,
    outer_output_weight,
    outer_product_bias,
):
    members = cluster_member_count.reshape(1, 64)
    count = sequence_block_count.reshape(1, 1)
    (packed,) = call(
        pack_kernel, [((8, 4, 8, 128), BF)], [VMEM], flops=1 << 30,
    )(alignment_rows)
    (bias_send,) = call(
        bias_kernel, [((64, 1, 128), F32)], [HBM] * 4,
        [((8, 128), BF), ((8, 128), F32), ((1, 64), jnp.int32), pltpu.SMEM((1,), jnp.int32),
         pltpu.SemaphoreType.DMA((4,))],
        limit=60,
    )(pair_features.reshape(8, 128), pair_bias_weight.T, members, sequence_block_count)
    bias_all = lax.all_to_all(bias_send, "seq", split_axis=0, concat_axis=0, tiled=True)
    bias_all = bias_all.reshape(64, 128)
    tables = call(
        weight_kernel,
        [((1024, 128), BF), ((1024, 512), BF), ((2, 192, 128), BF), ((2, 128, 64), BF),
         ((64, 128), BF), ((64, 32), BF), ((64, 128), BF), ((8, 128), F32), ((1, 512), F32),
         ((1, 512), F32), ((64, 128), F32), ((1, 256), F32)],
        [VMEM] * 8, flops=1 << 30,
    )(outer_output_weight, attention_in_weight, attention_out_weight, outer_factor_weight,
      outer_product_bias.reshape(1, 128), members, residue_present_mask.reshape(1, 64), count)
    outer_w, place, qvg_w, key_w, wide_w, left_w, right_w, shift, used, scale, absent, keep = tables
    send, inverse = call(
        send_kernel, [((8, 12, 8, 128), BF), ((8, 128), F32)], [VMEM] * 3,
    )(packed, bias_all, keep)
    rows_all = lax.all_to_all(send, "res", split_axis=0, concat_axis=0, tiled=True)
    (factor_send,) = call(
        attend_kernel, [((8, 22, 8, 128), BF)], [VMEM] * 10,
        [((64, 512), F32), ((2, 256, 64), BF), ((8, 64, 512), BF), ((8, 64, 64), BF),
         ((64, 512), F32), ((256, 128), F32), ((512, 128), F32)],
    )(rows_all, place, qvg_w, key_w, wide_w, left_w, right_w, used, scale, absent)
    factor_all = lax.all_to_all(factor_send, "res", split_axis=0, concat_axis=0, tiled=True)
    (partial,) = call(
        outer_kernel, [((64, 8, 128), BF)], [VMEM] * 3, [((512, 1024), BF), ((512, 128), F32)],
    )(keep, factor_all, outer_w)
    arrived = lax.all_to_all(partial, "seq", split_axis=0, concat_axis=0, tiled=True)
    row_attention_update, pair_update = call(
        finish_kernel, [((64, 8, 64), BF), ((1, 8, 128), BF)], [VMEM] * 4,
    )(arrived, factor_all, inverse, shift)
    return (row_attention_update, pair_update)


def solution(mesh):
    return jax.shard_map(
        local,
        mesh=mesh,
        in_specs=(
            P("seq", "res", None),
            P("res", "seq", None),
            P("seq"),
            P("seq"),
            P(),
            P(),
            P(),
            P(),
            P(),
            P(),
            P(),
        ),
        out_specs=(P("seq", "res", None), P("seq", "res", None)),
        check_vma=False,
    )
```
